32 devices in a mesh: lev: 2 (over x), lat: 16 (over z, y, core).
Axes of the slice: x: 2, y: 2, z: 4, core: 2. Of those that a mesh axis runs over, the one named last changes fastest.
Arguments:
- tokens: bfloat16 [8, 96, 24, 512], P('lev', 'lat'), may hold values from -6 to 6
- level_ids: int32 [8], P('lev'), may hold values from 0 to 12
- level_table: float32 [13, 512], replicated, may hold values from -6 to 6
- latent_query: bfloat16 [4, 512], replicated, may hold values from -360 to 360
- w_query: bfloat16 [512, 512], replicated, may hold values from -0.25 to 0.25
- w_kv: bfloat16 [512, 1024], replicated, may hold values from -0.25 to 0.25
- w_attn_out: bfloat16 [512, 512], replicated, may hold values from -0.25 to 0.25
- regions: int32 [96, 24, 4], P('lat', 'lev'), may hold values from 0 to 3
- gain_one: float32 [2, 512], replicated, may hold values from 0.25 to 1.75
- gain_two: float32 [2, 512], replicated, may hold values from 0.25 to 1.75
- w_qkv: bfloat16 [2, 512, 1536], P(None, 'lat'), may hold values from -0.25 to 0.25
- w_proj: bfloat16 [2, 512, 512], P(None, 'lat'), may hold values from -0.25 to 0.25
- w_up: bfloat16 [2, 512, 2048], P(None, 'lat'), may hold values from -0.25 to 0.25
- w_down: bfloat16 [2, 2048, 512], P(None, 'lat'), may hold values from -0.125 to 0.125
Outputs:
- grid_out: bfloat16 [96, 24, 4, 512], P('lat', 'lev')
The draws below stay inside these ranges and needn't reach their ends.
Inputs may be any that keep to these rules, and one draw needn't show every extreme that they name: `regions`: within a window of the shifted grid, tokens attend only to tokens of the same region id.
All inputs are finite; a program needn't handle non-finite values.
Results may differ from the reference program's by a relative error of at most 0.018.
Values may be sent and summed in bfloat16 or wider, within the bound.
No kernel may reach another device: no remote copies, remote signals or barrier semaphores. Data moves between devices by JAX's collectives and lax.ppermute only.
A program may use at most 64 MiB of HBM per device.

```python
import jax
import jax.numpy as jnp
from jax import lax

D = 512
HEADS = 16
HD = 32
FF = 2048
Q_LAT = 4
PRESSURE = 13
ROWS_DEV = 6
BLOCKS = 2
LEVELS = 8
H = 96
W = 24
N_LAT = 16


def draw_latent_query(key, part):
    base = jnp.clip(jax.random.normal(key, (Q_LAT, D), jnp.float32), -6.0, 6.0)
    return base.astype(jnp.bfloat16)


def plant(array, key, low, largest):
    extent = array.shape
    index_at = [jax.random.randint(jax.random.fold_in(key, axis), (), 0, extent[axis]) for axis in range(len(extent))]
    array = array.at[tuple(index_at)].set(low)
    longest = extent.index(max(extent))
    index_at[longest] = (index_at[longest] + 1) % extent[longest]
    return array.at[tuple(index_at)].set(largest)


def block_levels(rng, extent, pieces, low, largest):
    factor_of = 1.0
    for position, parts in pieces:
        heights = jax.random.uniform(jax.random.fold_in(jax.random.fold_in(rng, 6), position), (parts,), jnp.float32, low / len(pieces), largest / len(pieces))
        factor_of = factor_of * jnp.repeat(jnp.exp(heights), extent[position] // parts).reshape((-1,) + (1,) * (len(extent) - 1 - position))
    return factor_of


def normal_values(key, shape, deviation, reach, pieces=(), kind=jnp.bfloat16):
    values = jax.random.normal(key, shape, jnp.float32) * deviation
    if len(pieces) > 0:
        values = block_levels(key, shape, pieces, -0.22, 0.18) * values
    return jnp.clip(values, min=-reach, max=reach).astype(kind)


def setup_inputs(seed: int = 0) -> dict:
    key_list = jax.random.split(jax.random.key(seed), 15)
    return {
        "tokens": normal_values(key_list[0], (LEVELS, H, W, D), 1.0, 6.0, ((0, 2), (1, 16))),
        "level_ids": plant(jax.random.randint(key_list[1], (LEVELS,), 0, PRESSURE), jax.random.fold_in(key_list[1], 1), 0, PRESSURE - 1).astype(jnp.int32),
        "level_table": normal_values(key_list[2], (PRESSURE, D), 1.0, 6.0, (), jnp.float32),
        "latent_query": draw_latent_query(jax.random.fold_in(key_list[14], 71), 0),
        "w_query": normal_values(key_list[4], (D, D), D ** -0.5, 0.25),
        "w_kv": normal_values(key_list[5], (D, 2 * D), D ** -0.5, 0.25),
        "w_attn_out": normal_values(key_list[6], (D, D), D ** -0.5, 0.25),
        "regions": plant(jax.random.randint(key_list[7], (H, W, Q_LAT), 0, 4), jax.random.fold_in(key_list[7], 1), 0, 3).astype(jnp.int32),
        "gain_one": jnp.clip(1.0 + 0.15 * jax.random.normal(key_list[8], (BLOCKS, D), jnp.float32), 0.25, 1.75),
        "gain_two": jnp.clip(1.0 + 0.15 * jax.random.normal(key_list[9], (BLOCKS, D), jnp.float32), 0.25, 1.75),
        "w_qkv": normal_values(key_list[10], (BLOCKS, D, 3 * D), D ** -0.5, 0.25, ((1, 16),)),
        "w_proj": normal_values(key_list[11], (BLOCKS, D, D), D ** -0.5, 0.25, ((1, 16),)),
        "w_up": normal_values(key_list[12], (BLOCKS, D, FF), D ** -0.5, 0.25, ((1, 16),)),
        "w_down": normal_values(key_list[13], (BLOCKS, FF, D), FF ** -0.5, 0.125, ((1, 16),)),
    }


eps = 1e-05

def layer_norm(flat, gain):
    mean = lax.optimization_barrier(jnp.mean(flat, -1, keepdims=True))
    centred = flat - mean
    var = lax.optimization_barrier(jnp.mean(centred * centred, -1, keepdims=True))
    return centred * lax.rsqrt(var + eps) * gain

def windows(grid):
    rows, cols, levels, width = grid.shape
    grid = grid.reshape(rows // 6, 6, cols // 12, 12, levels // 2, 2, width)
    grid = grid.transpose(0, 2, 4, 1, 3, 5, 6)
    return grid.reshape(-1, 144, width)

def unwindows(tiles, rows, cols, levels):
    width = tiles.shape[-1]
    tiles = tiles.reshape(rows // 6, cols // 12, levels // 2, 6, 12, 2, width)
    tiles = tiles.transpose(0, 3, 1, 4, 2, 5, 6)
    return tiles.reshape(rows, cols, levels, width)

def level_embed(level_ids, level_table):
    kinds = level_table.shape[0]
    onehot = (level_ids[:, None] == jnp.arange(kinds, dtype=jnp.int32)[None, :]).astype(jnp.float32)
    return jnp.dot(onehot, level_table, precision=lax.Precision.HIGHEST)

def swin_block(grid, regions, gain_a, gain_b, w_qkv, w_proj, w_up, w_down, masked):
    rows, cols, levels, width = grid.shape
    flat = grid.reshape(-1, width).astype(jnp.float32)
    normed = layer_norm(flat, gain_a).astype(jnp.bfloat16)
    qkv = jnp.dot(normed, w_qkv, preferred_element_type=jnp.float32).astype(jnp.bfloat16)
    tiles = windows(qkv.reshape(rows, cols, levels, 3 * width)).reshape(-1, 144, 3, HEADS, HD).astype(jnp.float32)
    score = jnp.einsum('nahe,nbhe->nhab', tiles[:, :, 0], tiles[:, :, 1]) * HD ** (-0.5)
    if masked:
        idents = windows(regions[..., None])[..., 0]
        same = idents[:, :, None] == idents[:, None, :]
        score = jnp.where(same[:, None], score, -1000000000.0)
    top = lax.optimization_barrier(jnp.max(score, -1, keepdims=True))
    weight = jnp.exp(score - top)
    weight = (weight / lax.optimization_barrier(jnp.sum(weight, -1, keepdims=True))).astype(jnp.bfloat16)
    context = jnp.einsum('nhab,nbhe->nahe', weight.astype(jnp.float32), tiles[:, :, 2]).astype(jnp.bfloat16)
    context = unwindows(context.reshape(-1, 144, width), rows, cols, levels).reshape(-1, width)
    mixed = (flat + jnp.dot(context, w_proj, preferred_element_type=jnp.float32)).astype(jnp.bfloat16)
    normed_b = layer_norm(mixed.astype(jnp.float32), gain_b).astype(jnp.bfloat16)
    hidden = jax.nn.gelu(jnp.dot(normed_b, w_up, preferred_element_type=jnp.float32)).astype(jnp.bfloat16)
    result = mixed.astype(jnp.float32) + jnp.dot(hidden, w_down, preferred_element_type=jnp.float32)
    return result.astype(jnp.bfloat16).reshape(rows, cols, levels, width)

def reference(tokens, level_ids, level_table, latent_query, w_query, w_kv, w_attn_out, regions, gain_one, gain_two, w_qkv, w_proj, w_up, w_down):
    embed = level_embed(level_ids, level_table)
    queries = jnp.dot(latent_query, w_query, preferred_element_type=jnp.float32).astype(jnp.bfloat16)
    heads_q = queries.reshape(Q_LAT, HEADS, HD).astype(jnp.float32)

    def encode(band):
        start = (band * ROWS_DEV).astype(jnp.int32)
        piece = lax.dynamic_slice_in_dim(tokens, start, ROWS_DEV, 1)
        summed = (piece.astype(jnp.float32) + embed[:, None, None, :]).astype(jnp.bfloat16)
        kv = jnp.dot(summed.reshape(-1, D), w_kv, preferred_element_type=jnp.float32).astype(jnp.bfloat16)
        kv = kv.reshape(LEVELS, ROWS_DEV, W, 2, HEADS, HD).astype(jnp.float32)
        score = jnp.einsum('qhe,lrwhe->rwqhl', heads_q, kv[:, :, :, 0]) * HD ** (-0.5)
        weight = jax.nn.softmax(score, axis=-1)
        attended = jnp.einsum('rwqhl,lrwhe->rwqhe', weight, kv[:, :, :, 1])
        attended = attended.astype(jnp.bfloat16).reshape(-1, D)
        projected = jnp.dot(attended, w_attn_out, preferred_element_type=jnp.float32).reshape(ROWS_DEV, W, Q_LAT, D)
        return (projected + queries.astype(jnp.float32)).astype(jnp.bfloat16)
    latent = lax.map(encode, jnp.arange(N_LAT, dtype=jnp.int32)).reshape(H, W, Q_LAT, D)

    def plain_slab(slab):
        return swin_block(slab, None, gain_one[0], gain_two[0], w_qkv[0], w_proj[0], w_up[0], w_down[0], False)
    plain = lax.map(plain_slab, latent.reshape(H // 6, 6, W, Q_LAT, D)).reshape(H, W, Q_LAT, D)
    rolled = jnp.roll(plain, (-3, -6, -1), (0, 1, 2))

    def shifted_slab(pair):
        return swin_block(pair[0], pair[1], gain_one[1], gain_two[1], w_qkv[1], w_proj[1], w_up[1], w_down[1], True)
    shifted = lax.map(shifted_slab, (rolled.reshape(H // 6, 6, W, Q_LAT, D), regions.reshape(H // 6, 6, W, Q_LAT)))
    shifted = shifted.reshape(H, W, Q_LAT, D)
    return jnp.roll(shifted, (3, 6, 1), (0, 1, 2))
```

```python
import functools

import jax
import jax.numpy as jnp
import numpy as np
from jax import lax
from jax.experimental import pallas as pl
from jax.experimental.pallas import tpu as pltpu
from jax.sharding import PartitionSpec as P

HEADS = 16
HD = 32
Q_LAT = 4
WIN_ROWS = 6
WIN_COLS = 12
UNITS = 12
GROUP = 128 // HD

eps = 1e-05


BF = jnp.bfloat16
F32 = jnp.float32


def vspec():
    return pl.BlockSpec(memory_space=pltpu.VMEM)


def sspec():
    return pl.BlockSpec(memory_space=pltpu.SMEM)


def call(body, out_shape, args, smem=(), scratch=(), limit=None, name=None):
    many = isinstance(out_shape, (tuple, list))
    return pl.pallas_call(
        body,
        out_shape=out_shape,
        in_specs=[sspec() if i in smem else vspec() for i in range(len(args))],
        out_specs=[vspec() for _ in out_shape] if many else vspec(),
        scratch_shapes=list(scratch),
        compiler_params=pltpu.CompilerParams(vmem_limit_bytes=limit),
        name=name,
    )(*args)


def dot(a, b, dims=((1,), (0,))):
    return lax.dot_general(a, b, (dims, ((), ())), preferred_element_type=F32)


def layer_norm(flat, gain):
    mean = jnp.mean(flat, -1, keepdims=True)
    centred = flat - mean
    var = jnp.mean(centred * centred, -1, keepdims=True)
    return centred * lax.rsqrt(var + eps) * gain


def pack_body(lev, qkv, proj, up, down, *outs):
    width = proj.shape[-1]
    rows = proj.shape[1]
    blocks = proj.shape[0]
    for b in range(blocks):
        mine, other = outs[2 * b], outs[2 * b + 1]

        def fill(first, second, b=b):
            for u in range(3):
                first[u] = qkv[b, :, u * width : (u + 1) * width]
            first[3] = proj[b]
            for u in range(4):
                ref, at = (first, 4 + u) if u < 2 else (second, u - 2)
                ref[at] = up[b, :, u * width : (u + 1) * width]
            for u in range(4):
                second[2 + u] = down[b, u * rows : (u + 1) * rows, :]

        @pl.when(lev[0] == 0)
        def _():
            fill(mine, other)

        @pl.when(lev[0] != 0)
        def _():
            fill(other, mine)


def pack(lev, w_qkv, w_proj, w_up, w_down):
    blocks, rows, width = w_proj.shape
    half = jax.ShapeDtypeStruct((UNITS // 2, rows, width), BF)
    return call(pack_body, [half] * (2 * blocks), (lev, w_qkv, w_proj, w_up, w_down), smem=(0,), name="pack")


def over(axis, fn, array):
    return lax.ppermute(array, axis, [(i, fn(i)) for i in range(lax.axis_size(axis))])


def gather(mine, other):
    size = lax.axis_size("lat")
    lat = lax.axis_index("lat")
    outer = size // 4
    order = [0] + list(range(1, outer, 2)) + list(range(2, outer, 2))[::-1]
    place = {z: i for i, z in enumerate(order)}
    following = [order[(place[z] + 1) % outer] for z in range(outer)]
    before = [order[place[z] - 1] for z in range(outer)]
    back = jnp.asarray(before, jnp.int32)

    def ring(array):
        return over("lat", lambda i: following[i // 4] * 4 + i % 4, array)

    def flip(bit, array):
        return over("lat", lambda i: i ^ bit, array)

    def swap(array):
        return over("lev", lambda i: i ^ 1, array)

    got = [(mine, True, lat), (other, False, lat)]
    column = [(mine, lat)]
    for step in range(1, outer):
        array, at = column[-1]
        column.append((ring(array), back[at // 4] * 4 + at % 4))
    across = [(flip(2, array), at ^ 2) for array, at in column]
    got += [(array, True, at) for array, at in column[1:] + across]
    got.append((flip(2, other), False, lat ^ 2))
    if outer > 1:
        got.append((ring(other), False, column[1][1]))
    relay = [across[1:2], column[2:], across[2:]] if outer > 1 else []
    got += [(swap(array), False, at) for part in relay for array, at in part]
    return got + [(flip(1, array), kind, at ^ 1) for array, kind, at in got]


def prep_body(lev, ids, source, tokens, table, own, send):
    slots, rows, cols, width = tokens.shape
    count = rows * cols // 2
    lanes = lax.broadcasted_iota(jnp.int32, (count, rows * cols), 1)
    here = source[...] + lev[0] * (cols // 2)
    there = source[...] + (1 - lev[0]) * (cols // 2)
    pick_own = (lanes == here).astype(BF)
    pick_send = (lanes == there).astype(BF)
    for s in range(slots):
        level = table[pl.ds(ids[s], 1), :]
        summed = (tokens[s].reshape(rows * cols, width).astype(F32) + level).astype(BF)
        send[s] = dot(pick_send, summed).astype(BF)
        own[s] = dot(pick_own, summed).astype(BF)


def encode_body(own, recv, latent_query, w_query, w_kv, w_out, out, kv, weights):
    slots_half, count, width = own.shape
    slots = 2 * slots_half
    half_rows = slots_half * count
    kv[:half_rows, :] = dot(own[...].reshape(half_rows, width), w_kv[...]).astype(BF)
    kv[half_rows:, :] = dot(recv[...].reshape(half_rows, width), w_kv[...]).astype(BF)
    queries = dot(latent_query[...], w_query[...]).astype(BF).astype(F32)
    qh = Q_LAT * HEADS
    head_row = lax.broadcasted_iota(jnp.int32, (HEADS, width), 0)
    head_lane = lax.broadcasted_iota(jnp.int32, (HEADS, width), 1) // HD
    select = (head_row == head_lane).astype(F32)
    block = jnp.concatenate([queries[q : q + 1] * select for q in range(Q_LAT)], 0).astype(BF)
    score = dot(kv[:, :width], block, ((1,), (1,))) * HD ** (-0.5)
    score = score.reshape(slots, count, qh)
    top = jnp.max(score, 0)
    weight = jnp.exp(score - top[None])
    weight = (weight / jnp.sum(weight, 0)[None]).reshape(slots * count, qh)
    high = weight.astype(BF)
    low = (weight - high.astype(F32)).astype(BF)
    weights[...] = jnp.concatenate([high, low], 1)
    row = lax.broadcasted_iota(jnp.int32, (2 * qh, width), 0)
    lane = lax.broadcasted_iota(jnp.int32, (2 * qh, width), 1) // HD
    for q in range(Q_LAT):
        spread = ((row == lane + q * HEADS) | (row == lane + q * HEADS + qh)).astype(BF)
        total = None
        for s in range(slots):
            at = slice(s * count, (s + 1) * count)
            part = dot(weights[at, :], spread) * kv[at, width:].astype(F32)
            total = part if total is None else total + part
        attended = total.astype(BF)
        out[q * count : (q + 1) * count, :] = (dot(attended, w_out[...]) + queries[q : q + 1]).astype(BF)


def block_body(*refs, kinds, masked, tokens_in, out_count):
    at_ref, refs = refs[0], refs[1:]
    bufs, refs = refs[: len(kinds)], refs[len(kinds) :]
    gain_a, gain_b, refs = refs[0], refs[1], refs[2:]
    if masked:
        lab_row, lab_col, refs = refs[0], refs[1], refs[2:]
    ins, refs = refs[:tokens_in], refs[tokens_in:]
    outs, refs = refs[:out_count], refs[out_count:]
    w, x, ctx = refs
    width = x.shape[1]
    lat_size, rows = w.shape[0] // UNITS, w.shape[1]
    lev = at_ref[len(kinds)]
    for i, (buf, mine) in enumerate(zip(bufs, kinds)):
        j = at_ref[i]
        first = (lev == 0) if mine else (lev != 0)
        for u in range(UNITS // 2):
            index = u * lat_size + j
            if u < 2:
                other = (6 + u) * lat_size + j
            else:
                other = 8 * lat_size + 4 * j + (u - 2)
            w[jnp.where(first, index, other)] = buf[u]

    def weight(unit, count=1):
        part = w[unit * lat_size : (unit + count) * lat_size]
        return part.reshape(count * lat_size * rows, width)

    if masked:
        piece = ins[0].shape[0] // 4
        for q in range(4):
            value = ins[q][...].astype(F32)
            x[q * 2 * piece : (q + 1) * 2 * piece, :] = value[piece : 3 * piece]
            base = 8 * piece + q * 2 * piece
            x[base : base + piece, :] = value[3 * piece :]
            x[base + piece : base + 2 * piece, :] = value[:piece]
    else:
        x[...] = ins[0][...].astype(F32)
    total = x.shape[0]
    tokens = total // 2
    normed = layer_norm(x[...], gain_a[...]).astype(BF)
    query = dot(normed, weight(0)).astype(BF)
    keys = dot(normed, weight(1)).astype(BF)
    vals = dot(normed, weight(2)).astype(BF)
    lane = lax.broadcasted_iota(jnp.int32, (tokens, 128), 1) // HD
    zero = jnp.zeros((tokens, 128), BF)
    for n in range(2):
        if masked:
            same = lab_col[n] == lab_row[n]
        for g in range(width // 128):
            at = (slice(n * tokens, (n + 1) * tokens), slice(g * 128, (g + 1) * 128))
            q_g, k_g, v_g = query[at], keys[at], vals[at]
            weights, spread = [], []
            for h in range(GROUP):
                inside = lane == h
                k_h = jnp.where(inside, k_g, zero)
                score = dot(k_h, q_g, ((1,), (1,))) * HD ** (-0.5)
                if masked:
                    score = jnp.where(same, score, -1000000000.0)
                top = jnp.max(score, 0, keepdims=True)
                part = jnp.exp(score - top)
                part = part * (1.0 / jnp.sum(part, 0, keepdims=True))
                weights.append(part.astype(BF))
                spread.append(jnp.where(inside, v_g, zero))
            weights = jnp.concatenate(weights, 0)
            spread = jnp.concatenate(spread, 0)
            context = dot(spread, weights, ((0,), (0,)))
            ctx[at] = context.T.astype(BF)
    mixed = (x[...] + dot(ctx[...], weight(3))).astype(BF).astype(F32)
    normed_b = layer_norm(mixed, gain_b[...]).astype(BF)
    result = mixed
    down_all = w[8 * lat_size :].reshape(4 * width, width)
    for u in range(4):
        hidden = jax.nn.gelu(dot(normed_b, weight(4 + u))).astype(BF)
        result = result + dot(hidden, down_all[u * width : (u + 1) * width])
    result = result.astype(BF)
    x[...] = result.astype(F32)
    piece = total // 16
    if masked:
        for q in range(4):
            base = 8 * piece + q * 2 * piece
            parts = [
                x[base + piece : base + 2 * piece, :],
                x[q * 2 * piece : (q + 1) * 2 * piece, :],
                x[base : base + piece, :],
            ]
            outs[q][...] = jnp.concatenate(parts, 0).astype(BF)
    else:
        for q in range(4):
            parts = [x[(4 * k + q) * piece : (4 * k + q + 1) * piece, :] for k in range(Q_LAT)]
            outs[q][...] = jnp.concatenate(parts, 0).astype(BF)


def swin_block(got, gain_a, gain_b, tokens, labels, name):
    kinds = tuple(kind for _, kind, _ in got)
    at = jnp.stack([at for _, _, at in got] + [lax.axis_index("lev")]).astype(jnp.int32)
    bufs = [array for array, _, _ in got]
    rows, width = bufs[0].shape[1:]
    lat_size = lax.axis_size("lat")
    total = sum(t.shape[0] for t in tokens)
    args = [at] + bufs + [gain_a, gain_b] + list(labels) + list(tokens)
    body = functools.partial(
        block_body, kinds=kinds, masked=len(labels) > 0, tokens_in=len(tokens), out_count=4
    )
    quad = jax.ShapeDtypeStruct((total // 4, width), BF)
    scratch = [
        pltpu.VMEM((UNITS * lat_size, rows, width), BF),
        pltpu.VMEM((total, width), F32),
        pltpu.VMEM((total, width), BF),
    ]
    return call(body, [quad] * 4, args, smem=(0,), scratch=scratch, limit=40 << 20, name=name)


def roll_quarters(quarters, sign):
    size, sides = lax.axis_size("lat"), lax.axis_size("lev")
    pairs = [(i, (i + sign) % size) for i in range(size)]
    flat = [
        (a * size + i, ((a + sign) % sides) * size + (i + sign) % size) for a in range(sides) for i in range(size)
    ]
    one = lax.ppermute(quarters[1 if sign < 0 else 2], "lat", pairs)
    two = over("lev", lambda i: (i + sign) % sides, quarters[2 if sign < 0 else 1])
    three = lax.ppermute(quarters[0 if sign < 0 else 3], ("lev", "lat"), flat)
    if sign < 0:
        return quarters[3], two, one, three
    return three, one, two, quarters[0]


def unquarter_body(pick, *refs):
    quarters, out = refs[:4], refs[4]
    rows, cols, levels, width = out.shape
    stacked = jnp.concatenate([q[...] for q in quarters], 0)
    total = stacked.shape[0]
    lanes = lax.broadcasted_iota(jnp.int32, (total, total), 1)
    onehot = (lanes == pick[...]).astype(BF)
    flat = dot(onehot, stacked)
    for r in range(rows):
        for c in range(cols):
            at = (r * cols + c) * levels
            out[r, c] = flat[at : at + levels].astype(BF)


def quarter_order(rows, cols):
    grid = np.arange(rows * cols).reshape(2, rows // 2, 2, cols // 2)
    return grid.transpose(0, 2, 1, 3).reshape(-1)


def local(
    tokens,
    level_ids,
    level_table,
    latent_query,
    w_query,
    w_kv,
    w_attn_out,
    regions,
    gain_one,
    gain_two,
    w_qkv,
    w_proj,
    w_up,
    w_down,
):
    slots, rows, cols_all, width = tokens.shape
    cols = cols_all // lax.axis_size("lev")
    count = rows * cols
    lev = lax.axis_index("lev").astype(jnp.int32).reshape(1)
    packed = pack(lev, w_qkv, w_proj, w_up, w_down)
    order = quarter_order(rows, cols)
    source = jnp.asarray((order // cols * cols_all + order % cols).reshape(-1, 1), jnp.int32)
    part = jax.ShapeDtypeStruct((slots, count, width), BF)
    own, send = call(prep_body, [part, part], (lev, level_ids, source, tokens, level_table), smem=(0, 1), name="prep")
    recv = over("lev", lambda i: i ^ 1, send)
    state = call(
        encode_body,
        jax.ShapeDtypeStruct((Q_LAT * count, width), BF),
        (own, recv, latent_query, w_query, w_kv, w_attn_out),
        scratch=[pltpu.VMEM((2 * slots * count, 2 * width), BF), pltpu.VMEM((2 * slots * count, 128), BF)],
        name="encode",
    )
    labels = regions.reshape(2, rows // 2, 2, cols // 2, 2, 2).transpose(4, 0, 2, 5, 1, 3).reshape(2, -1)
    plain = swin_block(gather(packed[0], packed[1]), gain_one[:1], gain_two[:1], [state], (), "plain")
    rolled = roll_quarters(plain, -1)
    shifted = swin_block(
        gather(packed[2], packed[3]),
        gain_one[1:],
        gain_two[1:],
        rolled,
        (labels[:, None, :], labels[:, :, None]),
        "shifted",
    )
    quarters = roll_quarters(shifted, 1)
    inverse = np.argsort(order)
    per = count // 4
    where = inverse[:, None] // per * (Q_LAT * per) + np.arange(Q_LAT)[None] * per + inverse[:, None] % per
    pick = jnp.asarray(where.reshape(-1, 1), jnp.int32)
    return call(
        unquarter_body,
        jax.ShapeDtypeStruct((rows, cols, Q_LAT, width), BF),
        (pick,) + tuple(quarters),
        name="unquarter",
    )


def solution(mesh):
    in_specs = (
        P("lev", "lat", None, None),
        P("lev"),
        P(),
        P(),
        P(),
        P(),
        P(),
        P("lat", "lev", None),
        P(),
        P(),
        P(None, "lat", None),
        P(None, "lat", None),
        P(None, "lat", None),
        P(None, "lat", None),
    )
    out_specs = P("lat", "lev", None, None)
    return jax.shard_map(local, mesh=mesh, in_specs=in_specs, out_specs=out_specs, check_vma=False)
```

```python
import functools

import jax
import jax.numpy as jnp
import numpy as np
from jax import lax
from jax.experimental import pallas as pl
from jax.experimental.pallas import tpu as pltpu
from jax.sharding import PartitionSpec as P


HEADS = 16
HD = 32
Q_LAT = 4
UNITS = 12
GROUP = 128 // HD

eps = 1e-05


BF = jnp.bfloat16
F32 = jnp.float32


def vspec():
    return pl.BlockSpec(memory_space=pltpu.VMEM)


def sspec():
    return pl.BlockSpec(memory_space=pltpu.SMEM)


def call(body, out_shape, args, smem=(), alias=None, scratch=(), limit=8):
    many = isinstance(out_shape, (tuple, list))
    return pl.pallas_call(
        body,
        out_shape=out_shape,
        in_specs=[sspec() if i in smem else vspec() for i in range(len(args))],
        out_specs=[vspec() for _ in out_shape] if many else vspec(),
        scratch_shapes=list(scratch),
        compiler_params=pltpu.CompilerParams(vmem_limit_bytes=limit << 20),
        input_output_aliases=alias or {},
    )(*args)


def dot(a, b, dims=((1,), (0,))):
    return lax.dot_general(a, b, (dims, ((), ())), preferred_element_type=F32)


def layer_norm(flat, gain):
    mean = jnp.mean(flat, -1, keepdims=True)
    centred = flat - mean
    var = jnp.mean(centred * centred, -1, keepdims=True)
    return centred * lax.rsqrt(var + eps) * gain


def pack_body(qkv, proj, up, down, *outs):
    width = proj.shape[-1]
    rows = proj.shape[1]
    for b, out in enumerate(outs):
        for u in range(3):
            out[u] = qkv[b, :, u * width : (u + 1) * width]
        out[3] = proj[b]
        for u in range(4):
            out[4 + u] = up[b, :, u * width : (u + 1) * width]
            out[8 + u] = down[b, u * rows : (u + 1) * rows, :]


def pack(w_qkv, w_proj, w_up, w_down):
    blocks, rows, width = w_proj.shape
    own = jax.ShapeDtypeStruct((UNITS, rows, width), BF)
    return call(pack_body, [own] * blocks, (w_qkv, w_proj, w_up, w_down))


def over(axis, fn, array):
    return lax.ppermute(array, axis, [(i, fn(i)) for i in range(lax.axis_size(axis))])


def place_body(*refs, count):
    where, table, refs = refs[0], refs[1], refs[2:]
    bufs, w = refs[:count], refs[-1]
    lat_size = w.shape[0] // UNITS
    for i, buf in enumerate(bufs):
        j = table[i, where[1]]
        for u in range(UNITS):
            w[u * lat_size + j if u < 8 else 8 * lat_size + 4 * j + (u - 8)] = buf[u]


def place(where, w, group):
    rows, width = group[0][0].shape[1:]
    whole = jax.ShapeDtypeStruct((UNITS * lax.axis_size("lat"), rows, width), BF)
    table = jnp.asarray(np.stack([at for _, at in group]), jnp.int32)
    args = [where, table] + [array for array, _ in group]
    body = functools.partial(place_body, count=len(group))
    if w is None:
        return call(body, whole, args, smem=(0, 1), limit=2)
    return call(body, whole, args + [w], smem=(0, 1), limit=2, alias={len(args): 0})


def gather(where, own, tie):
    size = lax.axis_size("lat")
    outer = size // 4
    order = [0] + list(range(1, outer, 2)) + list(range(2, outer, 2))[::-1]
    spot = {z: i for i, z in enumerate(order)}
    following = [order[(spot[z] + 1) % outer] for z in range(outer)]
    before = np.array([order[spot[z] - 1] for z in range(outer)])
    at = np.arange(size)
    array, tied = own, own
    w = place(where, None, [(own, at)])
    waiting = [(over("lat", lambda i: i ^ 1, own), at ^ 1)]
    for step in range(outer):
        last = step == outer - 1
        if not last:
            ahead = over("lat", lambda i: following[i // 4] * 4 + i % 4, array)
        across = over("lat", lambda i: i ^ 2, tied)
        fresh = [(across, at ^ 2)]
        if step:
            fresh.append((over("lat", lambda i: i ^ 1, tied), at ^ 1))
        w = place(where, w, waiting + ([(tied, at)] if step else []))
        waiting = fresh + [(over("lat", lambda i: i ^ 1, across), at ^ 3)]
        if not last:
            array = ahead
            tied, w = lax.optimization_barrier((ahead, w))
            if step == outer - 2:
                tied, tie = lax.optimization_barrier((tied, tie))
            at = before[at // 4] * 4 + at % 4
    return place(where, w, waiting), tie


def prep_body(lev, ids, source, tokens, table, own, send):
    slots, rows, cols, width = tokens.shape
    count = rows * cols // 2
    lanes = lax.broadcasted_iota(jnp.int32, (count, rows * cols), 1)
    here = source[...] + lev[0] * (cols // 2)
    there = source[...] + (1 - lev[0]) * (cols // 2)
    pick_own = (lanes == here).astype(BF)
    pick_send = (lanes == there).astype(BF)
    for s in range(slots):
        level = table[pl.ds(ids[s], 1), :]
        summed = (tokens[s].reshape(rows * cols, width).astype(F32) + level).astype(BF)
        send[s] = dot(pick_send, summed).astype(BF)
        own[s] = dot(pick_own, summed).astype(BF)


def encode_body(own, recv, latent_query, w_query, w_kv, w_out, out, kv, weights):
    slots_half, count, width = own.shape
    slots = 2 * slots_half
    half_rows = slots_half * count
    kv[:half_rows, :] = dot(own[...].reshape(half_rows, width), w_kv[...]).astype(BF)
    kv[half_rows:, :] = dot(recv[...].reshape(half_rows, width), w_kv[...]).astype(BF)
    queries = dot(latent_query[...], w_query[...]).astype(BF).astype(F32)
    qh = Q_LAT * HEADS
    head_row = lax.broadcasted_iota(jnp.int32, (HEADS, width), 0)
    head_lane = lax.broadcasted_iota(jnp.int32, (HEADS, width), 1) // HD
    select = (head_row == head_lane).astype(F32)
    block = jnp.concatenate([queries[q : q + 1] * select for q in range(Q_LAT)], 0).astype(BF)
    score = dot(kv[:, :width], block, ((1,), (1,))) * HD ** (-0.5)
    score = score.reshape(slots, count, qh)
    top = jnp.max(score, 0)
    weight = jnp.exp(score - top[None])
    weight = (weight / jnp.sum(weight, 0)[None]).reshape(slots * count, qh)
    high = weight.astype(BF)
    low = (weight - high.astype(F32)).astype(BF)
    weights[...] = jnp.concatenate([high, low], 1)
    row = lax.broadcasted_iota(jnp.int32, (2 * qh, width), 0)
    lane = lax.broadcasted_iota(jnp.int32, (2 * qh, width), 1) // HD
    for q in range(Q_LAT):
        spread = ((row == lane + q * HEADS) | (row == lane + q * HEADS + qh)).astype(BF)
        total = None
        for s in range(slots):
            at = slice(s * count, (s + 1) * count)
            part = dot(weights[at, :], spread) * kv[at, width:].astype(F32)
            total = part if total is None else total + part
        attended = total.astype(BF)
        out[q * count : (q + 1) * count, :] = (dot(attended, w_out[...]) + queries[q : q + 1]).astype(BF)


def block_body(*refs, masked, tokens_in, out_count):
    w, gain_a, gain_b, refs = refs[0], refs[1], refs[2], refs[3:]
    if masked:
        labels, refs = refs[0], refs[1:]
    ins, refs = refs[:tokens_in], refs[tokens_in:]
    outs, refs = refs[:out_count], refs[out_count:]
    x, ctx = refs
    width = x.shape[1]
    lat_size = w.shape[0] // UNITS

    def weight(unit, count=1):
        return w[unit * lat_size : (unit + count) * lat_size].reshape(count * width, width)

    if masked:
        piece = ins[0].shape[0] // 4
        for q in range(4):
            value = ins[q][...].astype(F32)
            x[q * 2 * piece : (q + 1) * 2 * piece, :] = value[piece : 3 * piece]
            base = 8 * piece + q * 2 * piece
            x[base : base + piece, :] = value[3 * piece :]
            x[base + piece : base + 2 * piece, :] = value[:piece]
    else:
        x[...] = ins[0][...].astype(F32)
    total = x.shape[0]
    tokens = total // 2
    normed = layer_norm(x[...], gain_a[...]).astype(BF)
    query = dot(normed, weight(0)).astype(BF)
    keys = dot(normed, weight(1)).astype(BF)
    vals = dot(normed, weight(2)).astype(BF)
    lane = lax.broadcasted_iota(jnp.int32, (tokens, 128), 1) // HD
    zero = jnp.zeros((tokens, 128), BF)
    for n in range(2):
        if masked:
            row = labels[n : n + 1, :].astype(F32)
            same = jnp.broadcast_to(row, (8, tokens)).T[:, :1] == row
        for g in range(width // 128):
            at = (slice(n * tokens, (n + 1) * tokens), slice(g * 128, (g + 1) * 128))
            q_g, k_g, v_g = query[at], keys[at], vals[at]
            weights, spread = [], []
            for h in range(GROUP):
                inside = lane == h
                k_h = jnp.where(inside, k_g, zero)
                score = dot(k_h, q_g, ((1,), (1,))) * HD ** (-0.5)
                if masked:
                    score = jnp.where(same, score, -1000000000.0)
                top = jnp.max(score, 0, keepdims=True)
                part = jnp.exp(score - top)
                part = part * (1.0 / jnp.sum(part, 0, keepdims=True))
                weights.append(part.astype(BF))
                spread.append(jnp.where(inside, v_g, zero))
            weights = jnp.concatenate(weights, 0)
            spread = jnp.concatenate(spread, 0)
            context = dot(spread, weights, ((0,), (0,)))
            ctx[at] = context.T.astype(BF)
    mixed = (x[...] + dot(ctx[...], weight(3))).astype(BF).astype(F32)
    normed_b = layer_norm(mixed, gain_b[...]).astype(BF)
    result = mixed
    down_all = weight(8, 4)
    for u in range(4):
        hidden = jax.nn.gelu(dot(normed_b, weight(4 + u))).astype(BF)
        result = result + dot(hidden, down_all[u * width : (u + 1) * width])
    result = result.astype(BF)
    x[...] = result.astype(F32)
    piece = total // 16
    if masked:
        for q in range(4):
            base = 8 * piece + q * 2 * piece
            parts = [
                x[base + piece : base + 2 * piece, :],
                x[q * 2 * piece : (q + 1) * 2 * piece, :],
                x[base : base + piece, :],
            ]
            outs[q][...] = jnp.concatenate(parts, 0).astype(BF)
    else:
        for q in range(4):
            parts = [x[(4 * k + q) * piece : (4 * k + q + 1) * piece, :] for k in range(Q_LAT)]
            outs[q][...] = jnp.concatenate(parts, 0).astype(BF)


def swin_block(w, gain_a, gain_b, tokens, labels):
    width = w.shape[-1]
    total = sum(t.shape[0] for t in tokens)
    args = [w, gain_a, gain_b] + list(labels) + list(tokens)
    body = functools.partial(block_body, masked=len(labels) > 0, tokens_in=len(tokens), out_count=4)
    quad = jax.ShapeDtypeStruct((total // 4, width), BF)
    scratch = [pltpu.VMEM((total, width), F32), pltpu.VMEM((total, width), BF)]
    return call(body, [quad] * 4, args, scratch=scratch, limit=10)


def roll_quarters(quarters, sign):
    size, sides = lax.axis_size("lat"), lax.axis_size("lev")
    pairs = [(i, (i + sign) % size) for i in range(size)]
    flat = [
        (a * size + i, ((a + sign) % sides) * size + (i + sign) % size) for a in range(sides) for i in range(size)
    ]
    one = lax.ppermute(quarters[1 if sign < 0 else 2], "lat", pairs)
    two = over("lev", lambda i: (i + sign) % sides, quarters[2 if sign < 0 else 1])
    three = lax.ppermute(quarters[0 if sign < 0 else 3], ("lev", "lat"), flat)
    if sign < 0:
        return quarters[3], two, one, three
    return three, one, two, quarters[0]


def unquarter_body(pick, *refs):
    quarters, out = refs[:4], refs[4]
    rows, cols, levels, _ = out.shape
    stacked = jnp.concatenate([q[...] for q in quarters], 0)
    total = stacked.shape[0]
    lanes = lax.broadcasted_iota(jnp.int32, (total, total), 1)
    onehot = (lanes == pick[...]).astype(BF)
    flat = dot(onehot, stacked)
    for r in range(rows):
        for c in range(cols):
            at = (r * cols + c) * levels
            out[r, c] = flat[at : at + levels].astype(BF)


def quarter_order(rows, cols):
    grid = np.arange(rows * cols).reshape(2, rows // 2, 2, cols // 2)
    return grid.transpose(0, 2, 1, 3).reshape(-1)


def local(
    tokens,
    level_ids,
    level_table,
    latent_query,
    w_query,
    w_kv,
    w_attn_out,
    regions,
    gain_one,
    gain_two,
    w_qkv,
    w_proj,
    w_up,
    w_down,
):
    slots, rows, cols_all, width = tokens.shape
    cols = cols_all // lax.axis_size("lev")
    count = rows * cols
    lev = lax.axis_index("lev").astype(jnp.int32).reshape(1)
    where = jnp.stack([lax.axis_index("lev"), lax.axis_index("lat")]).astype(jnp.int32)
    packed = pack(w_qkv, w_proj, w_up, w_down)
    order = quarter_order(rows, cols)
    source = jnp.asarray((order // cols * cols_all + order % cols).reshape(-1, 1), jnp.int32)
    part = jax.ShapeDtypeStruct((slots, count, width), BF)
    own, send = call(prep_body, [part, part], (lev, level_ids, source, tokens, level_table), smem=(0, 1))
    recv = over("lev", lambda i: i ^ 1, send)
    state = call(
        encode_body,
        jax.ShapeDtypeStruct((Q_LAT * count, width), BF),
        (own, recv, latent_query, w_query, w_kv, w_attn_out),
        scratch=[pltpu.VMEM((2 * slots * count, 2 * width), BF), pltpu.VMEM((2 * slots * count, 128), BF)],
        limit=16,
    )
    labels = regions.reshape(2, rows // 2, 2, cols // 2, 2, 2).transpose(4, 0, 2, 5, 1, 3).reshape(2, -1)
    first, (state, labels) = gather(where, packed[0], (state, labels))
    plain = swin_block(first, gain_one[:1], gain_two[:1], [state], ())
    second, plain = gather(where, packed[1], tuple(plain))
    rolled = roll_quarters(plain, -1)
    shifted = swin_block(second, gain_one[1:], gain_two[1:], rolled, (labels,))
    quarters = roll_quarters(shifted, 1)
    inverse = np.argsort(order)
    per = count // 4
    where = inverse[:, None] // per * (Q_LAT * per) + np.arange(Q_LAT)[None] * per + inverse[:, None] % per
    pick = jnp.asarray(where.reshape(-1, 1), jnp.int32)
    return call(unquarter_body, jax.ShapeDtypeStruct((rows, cols, Q_LAT, width), BF), (pick,) + tuple(quarters))


def solution(mesh):
    in_specs = (
        P("lev", "lat", None, None),
        P("lev"),
        P(),
        P(),
        P(),
        P(),
        P(),
        P("lat", "lev", None),
        P(),
        P(),
        P(None, "lat", None),
        P(None, "lat", None),
        P(None, "lat", None),
        P(None, "lat", None),
    )
    out_specs = P("lat", "lev", None, None)

    return jax.shard_map(local, mesh=mesh, in_specs=in_specs, out_specs=out_specs, check_vma=False)
```

```python
import functools

import jax
import jax.numpy as jnp
import numpy as np
from jax import lax
from jax.experimental import pallas as pl
from jax.experimental.pallas import tpu as pltpu
from jax.sharding import PartitionSpec as P


HEADS = 16
HD = 32
Q_LAT = 4
UNITS = 12
GROUP = 128 // HD

eps = 1e-05


BF = jnp.bfloat16
F32 = jnp.float32


def vspec():
    return pl.BlockSpec(memory_space=pltpu.VMEM)


def sspec():
    return pl.BlockSpec(memory_space=pltpu.SMEM)


def call(body, out_shape, args, smem=(), alias=None, scratch=(), limit=8):
    many = isinstance(out_shape, (tuple, list))
    return pl.pallas_call(
        body,
        out_shape=out_shape,
        in_specs=[sspec() if i in smem else vspec() for i in range(len(args))],
        out_specs=[vspec() for _ in out_shape] if many else vspec(),
        scratch_shapes=list(scratch),
        compiler_params=pltpu.CompilerParams(vmem_limit_bytes=limit << 20),
        input_output_aliases=alias or {},
    )(*args)


def dot(a, b, dims=((1,), (0,))):
    return lax.dot_general(a, b, (dims, ((), ())), preferred_element_type=F32)


def layer_norm(flat, gain):
    mean = jnp.mean(flat, -1, keepdims=True)
    centred = flat - mean
    var = jnp.mean(centred * centred, -1, keepdims=True)
    return centred * lax.rsqrt(var + eps) * gain


def pack_body(qkv, proj, up, down, *outs):
    width = proj.shape[-1]
    rows = proj.shape[1]
    for b, out in enumerate(outs):
        for u in range(3):
            out[u] = qkv[b, :, u * width : (u + 1) * width]
        out[3] = proj[b]
        for u in range(4):
            out[4 + u] = up[b, :, u * width : (u + 1) * width]
            out[8 + u] = down[b, u * rows : (u + 1) * rows, :]


def pack(w_qkv, w_proj, w_up, w_down):
    blocks, rows, width = w_proj.shape
    own = jax.ShapeDtypeStruct((UNITS, rows, width), BF)
    return call(pack_body, [own] * blocks, (w_qkv, w_proj, w_up, w_down))


def over(axis, fn, array):
    return lax.ppermute(array, axis, [(i, fn(i)) for i in range(lax.axis_size(axis))])


def place_body(*refs, count):
    where, table, refs = refs[0], refs[1], refs[2:]
    bufs, w = refs[:count], refs[-1]
    lat_size = w.shape[0] // UNITS
    for i, buf in enumerate(bufs):
        j = table[i, where[1]]
        for u in range(UNITS):
            w[u * lat_size + j if u < 8 else 8 * lat_size + 4 * j + (u - 8)] = buf[u]


def place(where, w, group):
    rows, width = group[0][0].shape[1:]
    whole = jax.ShapeDtypeStruct((UNITS * lax.axis_size("lat"), rows, width), BF)
    table = jnp.asarray(np.stack([at for _, at in group]), jnp.int32)
    args = [where, table] + [array for array, _ in group]
    body = functools.partial(place_body, count=len(group))
    if w is None:
        return call(body, whole, args, smem=(0, 1), limit=2)
    return call(body, whole, args + [w], smem=(0, 1), limit=2, alias={len(args): 0})


def gather(where, own, early=(), tie=()):
    size = lax.axis_size("lat")
    outer = size // 4
    order = [0] + list(range(1, outer, 2)) + list(range(2, outer, 2))[::-1]
    spot = {z: i for i, z in enumerate(order)}
    following = [order[(spot[z] + 1) % outer] for z in range(outer)]
    before = np.array([order[spot[z] - 1] for z in range(outer)])
    at = np.arange(size)
    array, tied = own, own
    w = place(where, None, [(own, at)])
    waiting = [(over("lat", lambda i: i ^ 1, own), at ^ 1)]
    for step in range(outer):
        last = step == outer - 1
        if not last:
            ahead = over("lat", lambda i: following[i // 4] * 4 + i % 4, array)
        across = over("lat", lambda i: i ^ 2, tied)
        fresh = [(across, at ^ 2)]
        if step:
            fresh.append((over("lat", lambda i: i ^ 1, tied), at ^ 1))
        w = place(where, w, waiting + ([(tied, at)] if step else []))
        if last:
            across, tie = lax.optimization_barrier((across, tie))
        waiting = fresh + [(over("lat", lambda i: i ^ 1, across), at ^ 3)]
        if not last:
            array = ahead
            tied, w = lax.optimization_barrier((ahead, w))
            if step == outer - 2:
                tied, early = lax.optimization_barrier((tied, early))
            at = before[at // 4] * 4 + at % 4
    return place(where, w, waiting), early, tie


def prep_body(lev, ids, source, tokens, table, own, send):
    slots, rows, cols, width = tokens.shape
    count = rows * cols // 2
    lanes = lax.broadcasted_iota(jnp.int32, (count, rows * cols), 1)
    here = source[...] + lev[0] * (cols // 2)
    there = source[...] + (1 - lev[0]) * (cols // 2)
    pick_own = (lanes == here).astype(BF)
    pick_send = (lanes == there).astype(BF)
    for s in range(slots):
        level = table[pl.ds(ids[s], 1), :]
        summed = (tokens[s].reshape(rows * cols, width).astype(F32) + level).astype(BF)
        send[s] = dot(pick_send, summed).astype(BF)
        own[s] = dot(pick_own, summed).astype(BF)


def encode_body(own, recv, latent_query, w_query, w_kv, w_out, out, kv, weights):
    slots_half, count, width = own.shape
    slots = 2 * slots_half
    half_rows = slots_half * count
    kv[:half_rows, :] = dot(own[...].reshape(half_rows, width), w_kv[...]).astype(BF)
    kv[half_rows:, :] = dot(recv[...].reshape(half_rows, width), w_kv[...]).astype(BF)
    queries = dot(latent_query[...], w_query[...]).astype(BF).astype(F32)
    qh = Q_LAT * HEADS
    head_row = lax.broadcasted_iota(jnp.int32, (HEADS, width), 0)
    head_lane = lax.broadcasted_iota(jnp.int32, (HEADS, width), 1) // HD
    select = (head_row == head_lane).astype(F32)
    block = jnp.concatenate([queries[q : q + 1] * select for q in range(Q_LAT)], 0).astype(BF)
    score = dot(kv[:, :width], block, ((1,), (1,))) * HD ** (-0.5)
    score = score.reshape(slots, count, qh)
    top = jnp.max(score, 0)
    weight = jnp.exp(score - top[None])
    weight = (weight / jnp.sum(weight, 0)[None]).reshape(slots * count, qh)
    high = weight.astype(BF)
    low = (weight - high.astype(F32)).astype(BF)
    weights[...] = jnp.concatenate([high, low], 1)
    row = lax.broadcasted_iota(jnp.int32, (2 * qh, width), 0)
    lane = lax.broadcasted_iota(jnp.int32, (2 * qh, width), 1) // HD
    for q in range(Q_LAT):
        spread = ((row == lane + q * HEADS) | (row == lane + q * HEADS + qh)).astype(BF)
        total = None
        for s in range(slots):
            at = slice(s * count, (s + 1) * count)
            part = dot(weights[at, :], spread) * kv[at, width:].astype(F32)
            total = part if total is None else total + part
        attended = total.astype(BF)
        out[q * count : (q + 1) * count, :] = (dot(attended, w_out[...]) + queries[q : q + 1]).astype(BF)


def block_body(*refs, masked, tokens_in, out_count):
    w, gain_a, gain_b, refs = refs[0], refs[1], refs[2], refs[3:]
    if masked:
        labels, refs = refs[0], refs[1:]
    ins, refs = refs[:tokens_in], refs[tokens_in:]
    outs, refs = refs[:out_count], refs[out_count:]
    x, ctx = refs
    width = x.shape[1]
    lat_size = w.shape[0] // UNITS

    def weight(unit, count=1):
        return w[unit * lat_size : (unit + count) * lat_size].reshape(count * width, width)

    if masked:
        piece = ins[0].shape[0] // 4
        for q in range(4):
            value = ins[q][...].astype(F32)
            x[q * 2 * piece : (q + 1) * 2 * piece, :] = value[piece : 3 * piece]
            base = 8 * piece + q * 2 * piece
            x[base : base + piece, :] = value[3 * piece :]
            x[base + piece : base + 2 * piece, :] = value[:piece]
    else:
        x[...] = ins[0][...].astype(F32)
    total = x.shape[0]
    tokens = total // 2
    normed = layer_norm(x[...], gain_a[...]).astype(BF)
    query = dot(normed, weight(0)).astype(BF)
    keys = dot(normed, weight(1)).astype(BF)
    vals = dot(normed, weight(2)).astype(BF)
    lane = lax.broadcasted_iota(jnp.int32, (tokens, 128), 1) // HD
    zero = jnp.zeros((tokens, 128), BF)
    for n in range(2):
        if masked:
            row = labels[n : n + 1, :].astype(F32)
            same = jnp.broadcast_to(row, (8, tokens)).T[:, :1] == row
        for g in range(width // 128):
            at = (slice(n * tokens, (n + 1) * tokens), slice(g * 128, (g + 1) * 128))
            q_g, k_g, v_g = query[at], keys[at], vals[at]
            weights, spread = [], []
            for h in range(GROUP):
                inside = lane == h
                k_h = jnp.where(inside, k_g, zero)
                score = dot(k_h, q_g, ((1,), (1,))) * HD ** (-0.5)
                if masked:
                    score = jnp.where(same, score, -1000000000.0)
                top = jnp.max(score, 0, keepdims=True)
                part = jnp.exp(score - top)
                part = part * (1.0 / jnp.sum(part, 0, keepdims=True))
                weights.append(part.astype(BF))
                spread.append(jnp.where(inside, v_g, zero))
            weights = jnp.concatenate(weights, 0)
            spread = jnp.concatenate(spread, 0)
            context = dot(spread, weights, ((0,), (0,)))
            ctx[at] = context.T.astype(BF)
    mixed = (x[...] + dot(ctx[...], weight(3))).astype(BF).astype(F32)
    normed_b = layer_norm(mixed, gain_b[...]).astype(BF)
    result = mixed
    down_all = weight(8, 4)
    for u in range(4):
        hidden = jax.nn.gelu(dot(normed_b, weight(4 + u))).astype(BF)
        result = result + dot(hidden, down_all[u * width : (u + 1) * width])
    result = result.astype(BF)
    x[...] = result.astype(F32)
    piece = total // 16
    if masked:
        for q in range(4):
            base = 8 * piece + q * 2 * piece
            parts = [
                x[base + piece : base + 2 * piece, :],
                x[q * 2 * piece : (q + 1) * 2 * piece, :],
                x[base : base + piece, :],
            ]
            outs[q][...] = jnp.concatenate(parts, 0).astype(BF)
    else:
        for q in range(4):
            parts = [x[(4 * k + q) * piece : (4 * k + q + 1) * piece, :] for k in range(Q_LAT)]
            outs[q][...] = jnp.concatenate(parts, 0).astype(BF)


def swin_block(w, gain_a, gain_b, tokens, labels):
    width = w.shape[-1]
    total = sum(t.shape[0] for t in tokens)
    args = [w, gain_a, gain_b] + list(labels) + list(tokens)
    body = functools.partial(block_body, masked=len(labels) > 0, tokens_in=len(tokens), out_count=4)
    quad = jax.ShapeDtypeStruct((total // 4, width), BF)
    scratch = [pltpu.VMEM((total, width), F32), pltpu.VMEM((total, width), BF)]
    return call(body, [quad] * 4, args, scratch=scratch, limit=10)


def roll_quarters(quarters, sign):
    size, sides = lax.axis_size("lat"), lax.axis_size("lev")
    pairs = [(i, (i + sign) % size) for i in range(size)]
    flat = [
        (a * size + i, ((a + sign) % sides) * size + (i + sign) % size) for a in range(sides) for i in range(size)
    ]
    one = lax.ppermute(quarters[1 if sign < 0 else 2], "lat", pairs)
    two = over("lev", lambda i: (i + sign) % sides, quarters[2 if sign < 0 else 1])
    three = lax.ppermute(quarters[0 if sign < 0 else 3], ("lev", "lat"), flat)
    if sign < 0:
        return quarters[3], two, one, three
    return three, one, two, quarters[0]


def unquarter_body(pick, *refs):
    quarters, out = refs[:4], refs[4]
    rows, cols, levels, _ = out.shape
    stacked = jnp.concatenate([q[...] for q in quarters], 0)
    total = stacked.shape[0]
    lanes = lax.broadcasted_iota(jnp.int32, (total, total), 1)
    onehot = (lanes == pick[...]).astype(BF)
    flat = dot(onehot, stacked)
    for r in range(rows):
        for c in range(cols):
            at = (r * cols + c) * levels
            out[r, c] = flat[at : at + levels].astype(BF)


def quarter_order(rows, cols):
    grid = np.arange(rows * cols).reshape(2, rows // 2, 2, cols // 2)
    return grid.transpose(0, 2, 1, 3).reshape(-1)


def local(
    tokens,
    level_ids,
    level_table,
    latent_query,
    w_query,
    w_kv,
    w_attn_out,
    regions,
    gain_one,
    gain_two,
    w_qkv,
    w_proj,
    w_up,
    w_down,
):
    slots, rows, cols_all, width = tokens.shape
    cols = cols_all // lax.axis_size("lev")
    count = rows * cols
    lev = lax.axis_index("lev").astype(jnp.int32).reshape(1)
    where = jnp.stack([lax.axis_index("lev"), lax.axis_index("lat")]).astype(jnp.int32)
    packed = pack(w_qkv, w_proj, w_up, w_down)
    order = quarter_order(rows, cols)
    source = jnp.asarray((order // cols * cols_all + order % cols).reshape(-1, 1), jnp.int32)
    part = jax.ShapeDtypeStruct((slots, count, width), BF)
    own, send = call(prep_body, [part, part], (lev, level_ids, source, tokens, level_table), smem=(0, 1))
    recv = over("lev", lambda i: i ^ 1, send)
    state = call(
        encode_body,
        jax.ShapeDtypeStruct((Q_LAT * count, width), BF),
        (own, recv, latent_query, w_query, w_kv, w_attn_out),
        scratch=[pltpu.VMEM((2 * slots * count, 2 * width), BF), pltpu.VMEM((2 * slots * count, 128), BF)],
        limit=16,
    )
    labels = regions.reshape(2, rows // 2, 2, cols // 2, 2, 2).transpose(4, 0, 2, 5, 1, 3).reshape(2, -1)
    first, (labels,), _ = gather(where, packed[0], early=(labels,))
    plain = swin_block(first, gain_one[:1], gain_two[:1], [state], ())
    second, _, plain = gather(where, packed[1], tie=tuple(plain))
    rolled = roll_quarters(plain, -1)
    shifted = swin_block(second, gain_one[1:], gain_two[1:], rolled, (labels,))
    quarters = roll_quarters(shifted, 1)
    inverse = np.argsort(order)
    per = count // 4
    where = inverse[:, None] // per * (Q_LAT * per) + np.arange(Q_LAT)[None] * per + inverse[:, None] % per
    pick = jnp.asarray(where.reshape(-1, 1), jnp.int32)
    return call(unquarter_body, jax.ShapeDtypeStruct((rows, cols, Q_LAT, width), BF), (pick,) + tuple(quarters))


def solution(mesh):
    in_specs = (
        P("lev", "lat", None, None),
        P("lev"),
        P(),
        P(),
        P(),
        P(),
        P(),
        P("lat", "lev", None),
        P(),
        P(),
        P(None, "lat", None),
        P(None, "lat", None),
        P(None, "lat", None),
        P(None, "lat", None),
    )
    out_specs = P("lat", "lev", None, None)

    return jax.shard_map(local, mesh=mesh, in_specs=in_specs, out_specs=out_specs, check_vma=False)
```
